32 devices in a mesh: grp: 4 (over z), seq: 8 (over y, x, core).
Axes of the slice: x: 2, y: 2, z: 4, core: 2. Of those that a mesh axis runs over, the one named last changes fastest.
Arguments:
- inputs: bfloat16 [8192, 1024], P(('grp', 'seq')), may hold values from -12 to 12
- noise: bfloat16 [8192, 1024], P(('grp', 'seq')), may hold values from -6 to 6
- cotangent: bfloat16 [8192, 1024], P(('grp', 'seq')), may hold values from -12 to 12
- lengths: int32 [4, 3], P('grp'), may hold values from 400 to 1024, as said below
- span_starts: int32 [4, 20], P('grp'), may hold values from 0 to 2038
- ffn1_gain: bfloat16 [1024], P('seq'), may hold values from 0.099609375 to 1.8984375
- ffn1_up: bfloat16 [1024, 4096], P('seq'), may hold values from -0.1875 to 0.1875
- ffn1_down: bfloat16 [4096, 1024], P('seq'), may hold values from -0.09375 to 0.09375
- att_gain: bfloat16 [1024], P('seq'), may hold values from 0.099609375 to 1.8984375
- qkv_weight: bfloat16 [1024, 3072], P('seq'), may hold values from -0.1875 to 0.1875
- out_weight: bfloat16 [1024, 1024], P('seq'), may hold values from -0.75 to 0.75
- rel_bias: bfloat16 [8, 32], P('seq'), may hold values from -4 to 4
- conv_gain: bfloat16 [1024], P('seq'), may hold values from 0.099609375 to 1.8984375
- point1_weight: bfloat16 [1024, 2048], P('seq'), may hold values from -0.1875 to 0.1875
- depth_weight: bfloat16 [5, 1024], P(None, 'seq'), may hold values from -2.5 to 2.5
- bn_gain: bfloat16 [1024], P('seq'), may hold values from 0.099609375 to 1.8984375
- bn_shift: bfloat16 [1024], P('seq'), may hold values from -3 to 3
- point2_weight: bfloat16 [1024, 1024], P('seq'), may hold values from -0.1875 to 0.1875
- ffn2_gain: bfloat16 [1024], P('seq'), may hold values from 0.099609375 to 1.8984375
- ffn2_up: bfloat16 [1024, 4096], P('seq'), may hold values from -0.1875 to 0.1875
- ffn2_down: bfloat16 [4096, 1024], P('seq'), may hold values from -0.09375 to 0.09375
- final_gain: bfloat16 [1024], P('seq'), may hold values from 0.099609375 to 1.8984375
Outputs:
- output: bfloat16 [8192, 1024], P(('grp', 'seq'))
- input_grad: bfloat16 [8192, 1024], P(('grp', 'seq'))
- ffn1_gain_grad: float32 [1024], P('seq')
- ffn1_up_grad: float32 [1024, 4096], P('seq')
- ffn1_down_grad: float32 [4096, 1024], P('seq')
- att_gain_grad: float32 [1024], P('seq')
- qkv_weight_grad: float32 [1024, 3072], P('seq')
- out_weight_grad: float32 [1024, 1024], P('seq')
- rel_bias_grad: float32 [8, 32], P('seq')
- conv_gain_grad: float32 [1024], P('seq')
- point1_weight_grad: float32 [1024, 2048], P('seq')
- depth_weight_grad: float32 [5, 1024], P(None, 'seq')
- bn_gain_grad: float32 [1024], P('seq')
- bn_shift_grad: float32 [1024], P('seq')
- point2_weight_grad: float32 [1024, 1024], P('seq')
- ffn2_gain_grad: float32 [1024], P('seq')
- ffn2_up_grad: float32 [1024, 4096], P('seq')
- ffn2_down_grad: float32 [4096, 1024], P('seq')
- final_gain_grad: float32 [1024], P('seq')
The draws below stay inside these ranges and needn't reach their ends.
Inputs may be any that keep to these rules, and one draw needn't show every extreme that they name: Each row holds 3 lengths that sum to 2048; each is at least 400, and exactly one in every row is 1024. `span_starts`: spans may intersect one another and utterance ends.
All inputs are finite; a program needn't handle non-finite values.
Results may differ from the reference program's by a relative error of at most 0.02.
Values may be sent and summed in bfloat16 or wider, within the bound.
A program may use at most 256 MiB of HBM per device.

```python
import jax
import jax.numpy as jnp
from jax import lax

D = 1024
FF = 4096
H = 8
KERNEL = 5
NBUCKET = 32
SPAN_LEN = 10
HEAD_DIM = 128
GROUP = 2048
TOKENS = 8192
UTT_MAX = 1024
UTT_MIN = 400
UTTS = 3
SPANS = 20
N_GRP = 4


def rising_rows(key):
    row_scale = 1.0 + 2.0 * jnp.arange(TOKENS, dtype=jnp.float32)[:, None] / TOKENS
    entries = jnp.clip(jax.random.normal(key, (TOKENS, D), jnp.float32), -4.0, 4.0)
    return entries * row_scale


def draw_inputs(key, part):
    return rising_rows(jax.random.fold_in(key, 11)).astype(jnp.bfloat16)


def draw_cotangent(key, part):
    return rising_rows(jax.random.fold_in(key, 23)).astype(jnp.bfloat16)


def draw_lengths(key, part):
    others = UTTS - 1
    extra = GROUP - UTT_MAX - others * UTT_MIN
    room = UTT_MAX - UTT_MIN
    even = extra // others
    spare = extra % others
    reach = max(0, min(even, room - even - 1))
    pairs = others // 2

    def one_row(row_key):
        first_key, second_key, third_key = jax.random.split(row_key, 3)
        delta = jax.random.randint(first_key, (pairs,), 0, reach + 1, dtype=jnp.int32)
        moves = jnp.concatenate([jnp.stack([delta, -delta], axis=1).reshape(-1), jnp.zeros((others % 2,), jnp.int32)])
        counter = jnp.arange(others, dtype=jnp.int32)
        shares = UTT_MIN + even + (counter < spare).astype(jnp.int32) + moves
        shuffled = jnp.take(shares, jax.random.permutation(third_key, others))
        place = jax.random.randint(second_key, (), 0, UTTS, dtype=jnp.int32)
        slots = jnp.arange(UTTS, dtype=jnp.int32)
        source = jnp.clip(jnp.where(slots < place, slots, slots - 1), 0, others - 1)
        return jnp.where(slots == place, UTT_MAX, jnp.take(shuffled, source)).astype(jnp.int32)
    return jax.vmap(one_row)(jax.random.split(jax.random.fold_in(key, 37), N_GRP)).astype(jnp.int32)


def with_ends(values, key, least, high):
    extent = values.shape
    index_at = [jax.random.randint(jax.random.fold_in(key, axis), (), 0, extent[axis]) for axis in range(len(extent))]
    values = values.at[tuple(index_at)].set(least)
    longest = extent.index(max(extent))
    index_at[longest] = (index_at[longest] + 1) % extent[longest]
    return values.at[tuple(index_at)].set(high)


def shard_levels(own_key, extent, pieces, low, high):
    factor_of, own = 1.0, jax.random.fold_in(own_key, 6)
    for dim, parts in pieces:
        heights = jnp.exp(jax.random.uniform(jax.random.fold_in(own, dim), (parts,), jnp.float32, low / len(pieces), high / len(pieces)))
        factor_of = factor_of * jnp.repeat(heights, extent[dim] // parts).reshape([-1 if axis == dim else 1 for axis in range(len(extent))])
    return factor_of


def bell_draw(rng, extent, width, limit, pieces=(), kind=jnp.bfloat16):
    values = width * jax.random.normal(rng, extent, jnp.float32)
    if pieces:
        values = values * shard_levels(rng, extent, pieces, -0.22, 0.18)
    return jnp.clip(values, -limit, limit).astype(kind)


def setup_inputs(seed: int = 0) -> dict:
    streams_of = jax.random.split(jax.random.key(seed), 23)
    return {
        "inputs": draw_inputs(jax.random.fold_in(streams_of[22], 71), 0),
        "noise": bell_draw(streams_of[1], (TOKENS, D), 1.0, 6.0, ((0, 32),)),
        "cotangent": draw_cotangent(jax.random.fold_in(streams_of[22], 71), 0),
        "lengths": draw_lengths(jax.random.fold_in(streams_of[22], 71), 0),
        "span_starts": with_ends(jax.random.randint(streams_of[4], (N_GRP, SPANS), 0, GROUP - SPAN_LEN + 1), jax.random.fold_in(streams_of[4], 1), 0, GROUP - SPAN_LEN).astype(jnp.int32),
        "ffn1_gain": jnp.clip(1.0 + 0.18 * jax.random.normal(streams_of[5], (D,), jnp.float32), 0.099609375, 1.8984375).astype(jnp.bfloat16),
        "ffn1_up": bell_draw(streams_of[6], (D, FF), D ** -0.5, 0.1875, ((0, 8),)),
        "ffn1_down": bell_draw(streams_of[7], (FF, D), FF ** -0.5, 0.09375, ((0, 8),)),
        "att_gain": jnp.clip(1.0 + 0.18 * jax.random.normal(streams_of[8], (D,), jnp.float32), 0.099609375, 1.8984375).astype(jnp.bfloat16),
        "qkv_weight": bell_draw(streams_of[9], (D, 3 * D), D ** -0.5, 0.1875, ((0, 8),)),
        "out_weight": bell_draw(streams_of[10], (D, D), (D // 16) ** -0.5, 0.75, ((0, 8),)),
        "rel_bias": bell_draw(streams_of[11], (H, NBUCKET), 1.0, 4.0, ((0, 8),)),
        "conv_gain": jnp.clip(1.0 + 0.18 * jax.random.normal(streams_of[12], (D,), jnp.float32), 0.099609375, 1.8984375).astype(jnp.bfloat16),
        "point1_weight": bell_draw(streams_of[13], (D, 2 * D), D ** -0.5, 0.1875, ((0, 8),)),
        "depth_weight": bell_draw(streams_of[14], (KERNEL, D), KERNEL ** -0.5, 2.5, ((1, 8),)),
        "bn_gain": jnp.clip(1.0 + 0.18 * jax.random.normal(streams_of[15], (D,), jnp.float32), 0.099609375, 1.8984375).astype(jnp.bfloat16),
        "bn_shift": bell_draw(streams_of[16], (D,), 0.5, 3.0, ((0, 8),)),
        "point2_weight": bell_draw(streams_of[17], (D, D), D ** -0.5, 0.1875, ((0, 8),)),
        "ffn2_gain": jnp.clip(1.0 + 0.18 * jax.random.normal(streams_of[18], (D,), jnp.float32), 0.099609375, 1.8984375).astype(jnp.bfloat16),
        "ffn2_up": bell_draw(streams_of[19], (D, FF), D ** -0.5, 0.1875, ((0, 8),)),
        "ffn2_down": bell_draw(streams_of[20], (FF, D), FF ** -0.5, 0.09375, ((0, 8),)),
        "final_gain": jnp.clip(1.0 + 0.18 * jax.random.normal(streams_of[21], (D,), jnp.float32), 0.099609375, 1.8984375).astype(jnp.bfloat16),
    }


@jax.custom_vjp
def low(v):
    return lax.optimization_barrier(v.astype(jnp.bfloat16)).astype(jnp.float32)

@jax.custom_vjp
def low_back(v):
    return v

def low_keep(v):
    return (low(v), None)

def low_pass(kept, grad):
    return (grad,)

def back_keep(v):
    return (v, None)

def back_low(kept, grad):
    return (low(grad),)
low.defvjp(low_keep, low_pass)
low_back.defvjp(back_keep, back_low)
epsilon = 1e-05
limits = (8, 16, 32, 64, 128, 256, 512, 1024)
highest = lax.Precision.HIGHEST

def bucket_of(distance):
    magnitude = jnp.abs(distance)
    result = jnp.minimum(magnitude, 7)
    for bound_at in limits:
        result = result + (magnitude >= bound_at).astype(jnp.int32)
    return (result + 16 * (distance > 0).astype(jnp.int32)).astype(jnp.int32)

def layer_norm(tensor, gain_vec):
    centred = tensor - lax.optimization_barrier(jnp.mean(tensor, axis=-1, keepdims=True))
    return centred * lax.rsqrt(lax.optimization_barrier(jnp.mean(centred * centred, axis=-1, keepdims=True)) + epsilon) * gain_vec

def matmul(left, right):
    return jnp.dot(left, right, precision=highest)

def feed_forward(hidden, gain_vec, up_proj, down_proj):
    normed = low(layer_norm(hidden, gain_vec))
    inner_act = low_back(matmul(normed, up_proj))
    active_low = low(jax.nn.silu(inner_act))
    return hidden + 0.5 * low_back(matmul(active_low, down_proj))

def group_attention(qkv_group, segment, table):
    queries = qkv_group[:, 0]
    keys_all = qkv_group[:, 1]
    values_all = qkv_group[:, 2]
    block_len = min(512, GROUP)
    scaling = HEAD_DIM ** (-0.5)

    def one_block(block_idx):
        first_row = block_idx * block_len
        query_b = lax.dynamic_slice_in_dim(queries, first_row, block_len, 0)
        seg_rows = lax.dynamic_slice_in_dim(segment, first_row, block_len, 0)
        rows_at = first_row + jnp.arange(block_len, dtype=jnp.int32)
        cols_at = jnp.arange(GROUP, dtype=jnp.int32)
        bias_mat = jnp.take(table, bucket_of(cols_at[None, :] - rows_at[:, None]), axis=1)
        scores = jnp.einsum('qhd,khd->hqk', query_b, keys_all, precision=highest) * scaling + bias_mat
        scores = low_back(scores)
        same_utt = (seg_rows[:, None] == segment[None, :])[None]
        scores = jnp.where(same_utt, scores, -1e+30)
        shifted = jnp.exp(scores - lax.optimization_barrier(jnp.max(scores, axis=-1, keepdims=True)))
        prob_vals = low(shifted / lax.optimization_barrier(jnp.sum(shifted, axis=-1, keepdims=True)))
        return jnp.einsum('hqk,khd->qhd', prob_vals, values_all, precision=highest)
    blocks = lax.map(jax.checkpoint(one_block), jnp.arange(GROUP // block_len, dtype=jnp.int32))
    return blocks.reshape(GROUP, H, HEAD_DIM)

def depthwise(glu_all, segment_all, tap_weights):
    padded = jnp.pad(glu_all, ((0, 0), (2, 2), (0, 0)))
    seg_pad = jnp.pad(segment_all, ((0, 0), (2, 2)), constant_values=-1)
    result = jnp.zeros_like(glu_all)
    for tap_at in range(KERNEL):
        same_utt = (seg_pad[:, tap_at:tap_at + GROUP] == segment_all)[..., None]
        result = result + tap_weights[tap_at] * jnp.where(same_utt, padded[:, tap_at:tap_at + GROUP], 0.0)
    return result

def reference(inputs, noise, cotangent, lengths, span_starts, ffn1_gain, ffn1_up, ffn1_down, att_gain, qkv_weight, out_weight, rel_bias, conv_gain, point1_weight, depth_weight, bn_gain, bn_shift, point2_weight, ffn2_gain, ffn2_up, ffn2_down, final_gain):
    utt_ends = jnp.cumsum(lengths, axis=1)
    places = jnp.arange(GROUP, dtype=jnp.int32)
    segment = lax.optimization_barrier(jnp.sum((places[None, :, None] >= utt_ends[:, None, :]).astype(jnp.int32), axis=2)).astype(jnp.int32)
    covered = jnp.any((places[None, :, None] >= span_starts[:, None, :]) & (places[None, :, None] < span_starts[:, None, :] + SPAN_LEN), axis=2).reshape(TOKENS)
    noise_full = noise.astype(jnp.float32)
    params = tuple((entry.astype(jnp.float32) for entry in (ffn1_gain, ffn1_up, ffn1_down, att_gain, qkv_weight, out_weight, rel_bias, conv_gain, point1_weight, depth_weight, bn_gain, bn_shift, point2_weight, ffn2_gain, ffn2_up, ffn2_down, final_gain)))

    def forward(frames, weights):
        gain_ffn1, up_one, down_one, gain_att, w_qkv, w_out, table, gain_conv, w_point1, w_depth, gain_bn, shift_bn, w_point2, gain_ffn2, up_two, down_two, gain_final = weights
        hidden_zero = jnp.where(covered[:, None], noise_full, frames)
        hidden_one = feed_forward(hidden_zero, gain_ffn1, up_one, down_one)
        att_in = low(layer_norm(hidden_one, gain_att))
        qkv_all = low(low_back(matmul(att_in, w_qkv))).reshape(N_GRP, GROUP, 3, H, HEAD_DIM)

        def attend_group(group_item):
            return group_attention(group_item[0], group_item[1], table)
        attended = lax.map(attend_group, (qkv_all, segment))
        attended = low(low_back(attended.reshape(TOKENS, D)))
        hidden_two = hidden_one + low_back(matmul(attended, w_out))
        conv_in = low(layer_norm(hidden_two, gain_conv))
        gated = low_back(matmul(conv_in, w_point1))
        glu_low = low(gated[:, :D] * jax.nn.sigmoid(gated[:, D:]))
        conv_out = low_back(depthwise(glu_low.reshape(N_GRP, GROUP, D), segment, w_depth).reshape(TOKENS, D))
        mean_c = lax.optimization_barrier(jnp.mean(conv_out, axis=0))
        centred = conv_out - mean_c
        var_c = lax.optimization_barrier(jnp.mean(centred * centred, axis=0))
        bn_value = centred * lax.rsqrt(var_c + epsilon) * gain_bn + shift_bn
        swished = low(jax.nn.silu(bn_value))
        hidden_three = hidden_two + low_back(matmul(swished, w_point2))
        hidden_four = feed_forward(hidden_three, gain_ffn2, up_two, down_two)
        return layer_norm(hidden_four, gain_final)
    result, pullback = jax.vjp(forward, inputs.astype(jnp.float32), params)
    grad_frames, gradients = pullback(cotangent.astype(jnp.float32))
    return (result.astype(jnp.bfloat16), grad_frames.astype(jnp.bfloat16), gradients[0], gradients[1], gradients[2], gradients[3], gradients[4], gradients[5], gradients[6], gradients[7], gradients[8], gradients[9], gradients[10], gradients[11], gradients[12], gradients[13], gradients[14], gradients[15], gradients[16])
```

```python
import functools

import jax
import jax.numpy as jnp
from jax import lax
from jax.experimental import pallas as pl
from jax.experimental.pallas import tpu as pltpu
from jax.sharding import PartitionSpec as P

KERNEL = 5
SPAN_LEN = 10
HEAD_DIM = 128
BLK = 256
REACH = 4
TILES = 2 * REACH + 1
LOG2E = 1.4426950408889634

epsilon = 1e-05
limits = (8, 16, 32, 64, 128, 256, 512, 1024)
highest = lax.Precision.HIGHEST
bf16 = jnp.bfloat16
f32 = jnp.float32


def bucket_of(distance):
    magnitude = jnp.abs(distance)
    result = jnp.minimum(magnitude, 7)
    for bound_at in limits:
        result = result + (magnitude >= bound_at).astype(jnp.int32)
    return result + 16 * (distance > 0).astype(jnp.int32)


def normalize(tensor, gain_vec):
    centred = tensor - jnp.mean(tensor, axis=-1, keepdims=True)
    factor = lax.rsqrt(jnp.mean(centred * centred, axis=-1, keepdims=True) + epsilon)
    normed = centred * factor
    return (normed * gain_vec, normed, factor)


def normalize_back(grad_out, normed, factor, gain_vec):
    grad_gain = jnp.sum(grad_out * normed, axis=0)
    scaled = grad_out * gain_vec
    grad_in = factor * (
        scaled
        - jnp.mean(scaled, axis=-1, keepdims=True)
        - normed * jnp.mean(scaled * normed, axis=-1, keepdims=True)
    )
    return (grad_in, grad_gain)


def contract(left, right, left_dim, right_dim):
    return lax.dot_general(
        left, right, (((left_dim,), (right_dim,)), ((), ())), preferred_element_type=f32
    )


def matmul(left, right):
    return contract(left, right, 1, 0)


def left_product(left, right):
    return contract(left, right, 0, 0)


def right_product(left, right):
    return contract(left, right, 1, 1)


def swish_slope(pre_act):
    sig_val = jax.nn.sigmoid(pre_act)
    return sig_val * (1.0 + pre_act * (1.0 - sig_val))


def masked_scores(q, k, tile, key_at, begin, end, scale):
    scores = right_product(k, q) * scale + tile
    return jnp.where((key_at >= begin) & (key_at < end), scores, -1e30)


def fill_tiles(line_ref, tiles_ref):
    for t in range(TILES):
        row = jnp.broadcast_to(line_ref[t : t + 1, :], (BLK, 2 * BLK))
        tiles_ref[t] = pltpu.roll(row, 0, 1, stride=1, stride_axis=0)[:, :BLK]


def attend_kernel(
    scale, low_ref, high_ref, q_ref, k_ref, v_ref, begin_ref, end_ref, line_ref,
    out_ref, lse_ref, tiles_ref,
):
    i = pl.program_id(0)

    @pl.when(i == 0)
    def _():
        fill_tiles(line_ref, tiles_ref)

    q = q_ref[...]
    begin = begin_ref[...]
    end = end_ref[...]
    row_at = lax.broadcasted_iota(jnp.int32, (BLK, BLK), 0)

    def step(j, carry):
        peak, total, acc = carry
        at = pl.multiple_of(j * BLK, BLK)
        keys = k_ref[pl.ds(at, BLK), :]
        scores = masked_scores(
            q, keys, tiles_ref[j - i + REACH], row_at + at, begin, end, scale
        )
        peak_new = jnp.maximum(peak, jnp.max(scores, axis=0, keepdims=True))
        probs = jnp.exp2(scores - peak_new)
        shrink = jnp.exp2(peak - peak_new)
        total = total * shrink + jnp.sum(probs, axis=0, keepdims=True)
        acc = acc * shrink + left_product(v_ref[pl.ds(at, BLK), :], probs.astype(bf16))
        return peak_new, total, acc

    first = (
        jnp.full((1, BLK), -1e30, f32),
        jnp.zeros((1, BLK), f32),
        jnp.zeros((HEAD_DIM, BLK), f32),
    )
    peak, total, acc = lax.fori_loop(low_ref[i], high_ref[i], step, first)
    out_ref[...] = (acc / total).T
    lse_ref[...] = peak + jnp.log2(total)


def attend_back_kernel(
    scale, plain, low_ref, high_ref, q_ref, k_ref, v_ref, go_ref, out_ref, lse_ref,
    begin_ref, end_ref, line_ref, grad_ref, diag_ref, tiles_ref, sums_ref, gk_ref, gv_ref,
):
    i = pl.program_id(0)

    @pl.when(i == 0)
    def _():
        fill_tiles(line_ref, tiles_ref)
        sums_ref[...] = jnp.zeros_like(sums_ref)
        gk_ref[...] = jnp.zeros_like(gk_ref)
        gv_ref[...] = jnp.zeros_like(gv_ref)

    q = q_ref[...]
    go = go_ref[...]
    begin = begin_ref[...]
    end = end_ref[...]
    lse = lse_ref[...]
    delta = lax.dot_general(
        jnp.ones((8, HEAD_DIM), f32), go.astype(f32) * out_ref[...],
        (((1,), (1,)), ((), ())), precision=highest, preferred_element_type=f32,
    )[0:1, :]
    row_at = lax.broadcasted_iota(jnp.int32, (BLK, BLK), 0)

    def step(j, gq):
        at = pl.multiple_of(j * BLK, BLK)
        rows = pl.ds(at, BLK)
        keys = k_ref[rows, :]
        scores = masked_scores(
            q, keys, tiles_ref[j - i + REACH], row_at + at, begin, end, scale
        )
        probs = jnp.exp2(scores - lse)
        gp = right_product(v_ref[rows, :], go)
        gs = (probs * (gp - delta)).astype(bf16)
        gv_ref[rows, :] += matmul(probs.astype(bf16), go)
        gk_ref[rows, :] += matmul(gs, q)
        sums_ref[j - i + REACH] += gs.astype(f32)
        return gq + left_product(gs, keys)

    gq = lax.fori_loop(low_ref[i], high_ref[i], step, jnp.zeros((BLK, HEAD_DIM), f32))
    grad_ref[pl.ds(pl.multiple_of(i * BLK, BLK), BLK), 0:HEAD_DIM] = (gq * plain).astype(bf16)

    @pl.when(i == pl.num_programs(0) - 1)
    def _():
        grad_ref[:, HEAD_DIM : 2 * HEAD_DIM] = (gk_ref[...] * plain).astype(bf16)
        grad_ref[:, 2 * HEAD_DIM :] = gv_ref[...].astype(bf16)
        back_at = lax.broadcasted_iota(jnp.int32, (BLK, 2 * BLK), 0)
        for t in range(TILES):
            wide = jnp.concatenate([sums_ref[t], jnp.zeros((BLK, BLK), f32)], axis=1)
            bit = 1
            while bit < BLK:
                moved = pltpu.roll(wide, 2 * BLK - bit, 1)
                wide = jnp.where((back_at // bit) % 2 == 1, moved, wide)
                bit *= 2
            diag_ref[t : t + 1, :] = jnp.sum(wide, axis=0, keepdims=True)
        diag_ref[TILES:, :] = jnp.zeros((16 - TILES, 2 * BLK), f32)


def column(at):
    return pl.BlockSpec((BLK, HEAD_DIM), lambda i, low, high: (i, at))


def whole(at, rows):
    return pl.BlockSpec((rows, HEAD_DIM), lambda i, low, high: (0, at))


def line_row():
    return pl.BlockSpec((1, BLK), lambda i, low, high: (0, i))


def fixed(shape):
    return pl.BlockSpec(shape, lambda i, low, high: (0, 0))


def attend(qkv, low, high, begin, end, line):
    rows = qkv.shape[0]
    scale = HEAD_DIM ** (-0.5) * LOG2E
    return pl.pallas_call(
        functools.partial(attend_kernel, scale),
        out_shape=(
            jax.ShapeDtypeStruct((rows, HEAD_DIM), f32),
            jax.ShapeDtypeStruct((1, rows), f32),
        ),
        grid_spec=pltpu.PrefetchScalarGridSpec(
            num_scalar_prefetch=2,
            grid=(rows // BLK,),
            in_specs=[
                column(0), whole(1, rows), whole(2, rows),
                line_row(), line_row(), fixed((16, 2 * BLK)),
            ],
            out_specs=(column(0), line_row()),
            scratch_shapes=[pltpu.VMEM((TILES, BLK, BLK), f32)],
        ),
        name="attend",
    )(low, high, qkv, qkv, qkv, begin, end, line)


def attend_back(qkv, grad_out, out, lse, low, high, begin, end, line):
    rows = qkv.shape[0]
    plain = HEAD_DIM ** (-0.5)
    return pl.pallas_call(
        functools.partial(attend_back_kernel, plain * LOG2E, plain),
        out_shape=(
            jax.ShapeDtypeStruct((rows, 3 * HEAD_DIM), bf16),
            jax.ShapeDtypeStruct((16, 2 * BLK), f32),
        ),
        grid_spec=pltpu.PrefetchScalarGridSpec(
            num_scalar_prefetch=2,
            grid=(rows // BLK,),
            in_specs=[
                column(0), whole(1, rows), whole(2, rows), column(0), column(0),
                line_row(), line_row(), line_row(), fixed((16, 2 * BLK)),
            ],
            out_specs=(fixed((rows, 3 * HEAD_DIM)), fixed((16, 2 * BLK))),
            scratch_shapes=[
                pltpu.VMEM((TILES, BLK, BLK), f32),
                pltpu.VMEM((TILES, BLK, BLK), f32),
                pltpu.VMEM((rows, HEAD_DIM), f32),
                pltpu.VMEM((rows, HEAD_DIM), f32),
            ],
        ),
        name="attend_back",
    )(low, high, qkv, qkv, qkv, grad_out, out, lse, begin, end, line)


def gather_rows(block):
    return lax.all_gather(block, "seq", axis=0, tiled=True)


def scatter_rows(partial):
    return lax.psum_scatter(
        partial.astype(bf16), "seq", scatter_dimension=0, tiled=True
    ).astype(f32)


def own_columns(weight, parts):
    count = lax.axis_size("seq")
    rows, width = weight.shape
    split = weight.reshape(rows, parts, count, width // (parts * count))
    moved = lax.all_to_all(split, "seq", split_axis=2, concat_axis=0, tiled=True)
    return moved.reshape(rows * count, width // count)


def own_rows(grad, parts):
    count = lax.axis_size("seq")
    rows, width = grad.shape
    split = grad.astype(bf16).reshape(rows, parts, 1, width // parts)
    moved = lax.all_to_all(split, "seq", split_axis=0, concat_axis=2, tiled=True)
    return moved.reshape(rows // count, width * count)


def grp_sum(value):
    return lax.psum(value.astype(bf16), "grp").astype(f32)


def per_device(
    inputs, noise, cotangent, lengths, span_starts,
    ffn1_gain, ffn1_up, ffn1_down, att_gain, qkv_weight, out_weight, rel_bias,
    conv_gain, point1_weight, depth_weight, bn_gain, bn_shift, point2_weight,
    ffn2_gain, ffn2_up, ffn2_down, final_gain,
):
    frame_count = inputs.shape[0]
    count = lax.axis_size("seq")
    groups = lax.axis_size("grp")
    group_len = frame_count * count
    total_len = group_len * groups
    offset = lax.axis_index("seq") * frame_count
    gains = lax.all_gather(
        jnp.stack([ffn1_gain, att_gain, conv_gain, ffn2_gain, final_gain]),
        "seq", axis=1, tiled=True,
    ).astype(f32)
    up_one = own_columns(ffn1_up, 1)
    w_qkv = own_columns(qkv_weight, 3)
    w_point1 = own_columns(point1_weight, 2)
    up_two = own_columns(ffn2_up, 1)

    ends = jnp.cumsum(lengths[0])
    starts = ends - lengths[0]
    places = jnp.arange(group_len, dtype=jnp.int32)
    inside = (places[:, None] >= starts[None, :]) & (places[:, None] < ends[None, :])
    begin = jnp.sum(jnp.where(inside, starts[None, :], 0), axis=1)
    end = jnp.sum(jnp.where(inside, ends[None, :], 0), axis=1)
    low = begin[::BLK] // BLK
    high = (end[BLK - 1 :: BLK] + BLK - 1) // BLK
    begin_row = begin[None, :]
    end_row = end[None, :]
    delta_at = (jnp.arange(16, dtype=jnp.int32) - REACH)[:, None] * BLK
    lane_at = jnp.arange(2 * BLK, dtype=jnp.int32)[None, :]
    lane_at = jnp.where(lane_at < BLK, lane_at, lane_at - 2 * BLK)
    bucket = bucket_of(delta_at - lane_at).reshape(-1)
    onehot = (bucket[None, :] == jnp.arange(rel_bias.shape[1], dtype=jnp.int32)[:, None]).astype(f32)
    line = jnp.dot(rel_bias.astype(f32) * LOG2E, onehot, precision=highest).reshape(16, 2 * BLK)

    local_at = offset + jnp.arange(frame_count, dtype=jnp.int32)
    begins = span_starts[0]
    covered = jnp.any(
        (local_at[:, None] >= begins[None, :]) & (local_at[:, None] < begins[None, :] + SPAN_LEN),
        axis=1,
    )[:, None]

    def ffn_forward(hidden, gain_vec, up_proj, down_proj):
        normal_out, normed, factor = normalize(hidden, gain_vec)
        full = gather_rows(normal_out.astype(bf16))
        pre_act = matmul(full, up_proj)
        inner = jax.nn.silu(pre_act).astype(bf16)
        result = hidden + 0.5 * scatter_rows(matmul(inner, down_proj))
        return result, (full, pre_act, inner, normed, factor)

    def ffn_backward(grad_h, saved, gain_vec, up_proj, down_proj):
        full, pre_act, inner, normed, factor = saved
        branch = gather_rows((0.5 * grad_h).astype(bf16))
        grad_down = left_product(inner, branch)
        grad_pre = (right_product(branch, down_proj) * swish_slope(pre_act)).astype(bf16)
        grad_up = left_product(full, grad_pre)
        grad_in, grad_gain = normalize_back(
            scatter_rows(right_product(grad_pre, up_proj)), normed, factor, gain_vec
        )
        return grad_h + grad_in, grad_gain, grp_sum(own_rows(grad_up, 1)), grp_sum(grad_down)

    hidden_zero = jnp.where(covered, noise.astype(f32), inputs.astype(f32))
    hidden_one, saved_one = ffn_forward(hidden_zero, gains[0], up_one, ffn1_down)

    att_out, att_normed, att_factor = normalize(hidden_one, gains[1])
    att_full = gather_rows(att_out.astype(bf16))
    qkv = matmul(att_full, w_qkv).astype(bf16)
    att_exact, lse = attend(qkv, low, high, begin_row, end_row, line)
    attended = att_exact.astype(bf16)
    hidden_two = hidden_one + scatter_rows(matmul(attended, out_weight))

    conv_out, conv_normed, conv_factor = normalize(hidden_two, gains[2])
    conv_full = gather_rows(conv_out.astype(bf16))
    gated = matmul(conv_full, w_point1)
    width = gated.shape[1] // 2
    linear_part = gated[:, :width]
    sig_gate = jax.nn.sigmoid(gated[:, width:])
    glu = (linear_part * sig_gate).astype(bf16).astype(f32)
    taps = depth_weight.astype(f32)

    def shifted(value, shift):
        at = places + shift
        same = ((at >= begin) & (at < end))[:, None]
        padded = jnp.pad(value, ((2, 2), (0, 0)))
        return jnp.where(same, padded[2 + shift : 2 + shift + group_len], 0.0)

    conv_sum = sum(taps[k] * shifted(glu, k - 2) for k in range(KERNEL))
    mean_c = lax.psum(jnp.sum(conv_sum, axis=0), "grp") / total_len
    centred = conv_sum - mean_c
    var_c = lax.psum(jnp.sum(centred * centred, axis=0), "grp") / total_len
    inv_std = lax.rsqrt(var_c + epsilon)
    normed_bn = centred * inv_std
    gain_bn = bn_gain.astype(f32)
    bn_value = normed_bn * gain_bn + bn_shift.astype(f32)
    swished = jax.nn.silu(bn_value).astype(bf16)
    hidden_three = hidden_two + scatter_rows(matmul(swished, point2_weight))

    hidden_four, saved_two = ffn_forward(hidden_three, gains[3], up_two, ffn2_down)
    final_out, final_normed, final_factor = normalize(hidden_four, gains[4])
    output = final_out.astype(bf16)

    grad_four, grad_gfinal = normalize_back(
        cotangent.astype(f32), final_normed, final_factor, gains[4]
    )
    grad_three, grad_gffn2, grad_up2, grad_down2 = ffn_backward(
        grad_four, saved_two, gains[3], up_two, ffn2_down
    )

    branch = gather_rows(grad_three.astype(bf16))
    grad_point2 = grp_sum(left_product(swished, branch))
    grad_bn = right_product(branch, point2_weight) * swish_slope(bn_value)
    grad_gain_bn, grad_shift_bn = lax.psum(
        (jnp.sum(grad_bn * normed_bn, axis=0), jnp.sum(grad_bn, axis=0)), "grp"
    )
    grad_conv = (
        inv_std
        * gain_bn
        * (grad_bn - grad_shift_bn / total_len - normed_bn * (grad_gain_bn / total_len))
    ).astype(bf16).astype(f32)
    grad_depth = jnp.stack(
        [jnp.sum(grad_conv * shifted(glu, k - 2), axis=0) for k in range(KERNEL)]
    )
    grad_glu = sum(taps[k] * shifted(grad_conv, 2 - k) for k in range(KERNEL))
    grad_gated = jnp.concatenate(
        [grad_glu * sig_gate, grad_glu * linear_part * sig_gate * (1.0 - sig_gate)], axis=1
    ).astype(bf16)
    grad_point1 = grp_sum(own_rows(left_product(conv_full, grad_gated), 2))
    grad_in3, grad_gconv = normalize_back(
        scatter_rows(right_product(grad_gated, w_point1)), conv_normed, conv_factor, gains[2]
    )
    grad_two = grad_three + grad_in3

    grad_att = gather_rows(grad_two.astype(bf16))
    grad_wout = grp_sum(left_product(attended, grad_att))
    grad_attended = right_product(grad_att, out_weight).astype(bf16)
    grad_qkv, diag = attend_back(
        qkv, grad_attended, att_exact, lse, low, high, begin_row, end_row, line
    )
    grad_table = jnp.dot(diag.reshape(1, -1), onehot.T, precision=highest)
    grad_wqkv = grp_sum(own_rows(left_product(att_full, grad_qkv), 3))
    grad_in2, grad_gatt = normalize_back(
        scatter_rows(right_product(grad_qkv, w_qkv)), att_normed, att_factor, gains[1]
    )
    grad_one = grad_two + grad_in2
    grad_zero, grad_gffn1, grad_up1, grad_down1 = ffn_backward(
        grad_one, saved_one, gains[0], up_one, ffn1_down
    )
    input_grad = jnp.where(covered, 0.0, grad_zero).astype(bf16)
    gain_grads = lax.psum_scatter(
        jnp.stack([grad_gffn1, grad_gatt, grad_gconv, grad_gffn2, grad_gfinal]),
        "seq", scatter_dimension=1, tiled=True,
    )
    gain_grads, grad_depth, grad_table = lax.psum((gain_grads, grad_depth, grad_table), "grp")
    return (
        output, input_grad, gain_grads[0], grad_up1, grad_down1, gain_grads[1], grad_wqkv,
        grad_wout, grad_table, gain_grads[2], grad_point1, grad_depth, grad_gain_bn,
        grad_shift_bn, grad_point2, gain_grads[3], grad_up2, grad_down2, gain_grads[4],
    )


def solution(mesh):
    rows, seq, flat = P(("grp", "seq"), None), P("seq", None), P("seq")
    table, taps, per_group = P("seq", None), P(None, "seq"), P("grp", None)
    return jax.shard_map(
        per_device,
        mesh=mesh,
        in_specs=(
            rows, rows, rows, per_group, per_group, flat, seq, seq, flat, seq, seq, table,
            flat, seq, taps, flat, flat, seq, flat, seq, seq, flat,
        ),
        out_specs=(
            rows, rows, flat, seq, seq, flat, seq, seq, table, flat, seq, taps, flat, flat,
            seq, flat, seq, seq, flat,
        ),
        check_vma=False,
    )
```
